32 devices in a mesh: lat: 2 (over y), lon: 8 (over z, core), freq: 2 (over x).
Axes of the slice: x: 2, y: 2, z: 4, core: 2. Of those that a mesh axis runs over, the one named last changes fastest.
Arguments:
- spectrum: float32 [36, 36, 8, 1024], P('freq', None, 'lat', 'lon'), may hold values from 0.05 to 1
- group_speed: float32 [36], P('freq'), may hold values from 0.15 to 0.6
- sea_mask: int32 [8, 1024], P('lat', 'lon'), may hold values 0 or 1
- wind_growth: float32 [8, 1024], P('lat', 'lon'), may hold values from 0.2 to 2
- dissipation: float32 [8, 1024], P('lat', 'lon'), may hold values from 0.1 to 1
- wind_profile: float32 [1296], replicated, may hold values from 0.02 to 0.2
- nonlinear_coef: float32 [1296], replicated, may hold values from 0.05 to 0.5
- momentum: float32 [2, 1296], replicated, may hold values from -6 to 6
- quadruplet: int32 [2, 1296], replicated, may hold values from 0 to 1295, as said below
- ocean_cell: int32 [8, 1024], P('lat', 'lon'), may hold values from 0 to 8191, as said below
Outputs:
- spectrum_out: float32 [36, 36, 8, 1024], P('freq', None, 'lat', 'lon')
- ocean_stress: float32 [8192, 2], P(('lon', 'freq'))
The draws below stay inside these ranges and needn't reach their ends.
Inputs may be any that keep to these rules, and one draw needn't show every extreme that they name: quadruplet[0, b] names a bin 1 or 2 frequencies higher (at most the highest) and 1 to 6 directions further, cyclically; quadruplet[1, b] one 1 or 2 frequencies lower (at least the lowest) and 1 to 6 directions back. ocean_cell[i, j] = j * 8 + i2 with i2 within 1 of i.
All inputs are finite; a program needn't handle non-finite values. No bound on the sum of `sea_mask` on one device may be relied on, other than what follows from the above.
Results may differ from the reference program's by a relative error of at most 0.000094.
Values sent between devices are 32-bit elements; how exact they have to be, the bound alone decides.
A program may use at most 64 MiB of HBM per device.

```python
import math
import jax
import jax.numpy as jnp
from jax import lax

NF = 36
NDIR = 36
NB = 1296
NLAT = 8
NLON = 1024
OCELLS = 8192


def draw_quadruplet(key, part):
    keys = jax.random.split(jax.random.fold_in(key, 7), 4)
    bins = jnp.arange(NF * NDIR)
    freqs = bins // NDIR
    directions = bins % NDIR
    up_freq = jax.random.randint(keys[0], (NF * NDIR,), 1, 3)
    up_dir = jax.random.randint(keys[1], (NF * NDIR,), 1, 7)
    down_freq = jax.random.randint(keys[2], (NF * NDIR,), 1, 3)
    down_dir = jax.random.randint(keys[3], (NF * NDIR,), 1, 7)
    higher = jnp.minimum(freqs + up_freq, NF - 1) * NDIR + (directions + up_dir) % NDIR
    lower = jnp.maximum(freqs - down_freq, 0) * NDIR + (directions - down_dir + NDIR) % NDIR
    return jnp.stack([higher, lower]).astype(jnp.int32)


def draw_ocean_cell(key, part):
    jitter = jax.random.randint(jax.random.fold_in(key, 11), (NLAT, NLON), -1, 2)
    lat_rows = jnp.arange(NLAT)[:, None]
    lon_cols = jnp.arange(NLON)[None, :]
    shifted = jnp.clip(lat_rows + jitter, 0, NLAT - 1)
    return (lon_cols * NLAT + shifted).astype(jnp.int32)


def place_ends(values, key, low, top_value):
    spot = [jax.random.randint(jax.random.fold_in(key, axis), (), 0, length) for axis, length in enumerate(values.shape)]
    main_axis = values.shape.index(max(values.shape))
    next_to = spot[:main_axis] + [(spot[main_axis] + 1) % values.shape[main_axis]] + spot[main_axis + 1:]
    return values.at[tuple(spot)].set(low).at[tuple(next_to)].set(top_value)


def steps_of(rng, extent, pieces, least, top_value):
    level, own = 1.0, jax.random.fold_in(rng, 6)
    for axis_at, shards_of in pieces:
        heights = jnp.exp(jax.random.uniform(jax.random.fold_in(own, axis_at), (shards_of,), jnp.float32, least / len(pieces), top_value / len(pieces)))
        level = level * jnp.repeat(heights, extent[axis_at] // shards_of).reshape([-1 if axis == axis_at else 1 for axis in range(len(extent))])
    return level


def noise(key, shape, deviation, reach, dtype=jnp.bfloat16):
    values = deviation * jax.random.normal(key, shape, jnp.float32)
    return jnp.clip(values, min=-reach, max=reach).astype(dtype)


def setup_inputs(seed: int = 0) -> dict:
    splits = jax.random.split(jax.random.key(seed), 11)
    spectrum = jnp.clip(0.05 + 0.95 * jax.random.uniform(splits[0], (NF, NDIR, NLAT, NLON), jnp.float32) ** steps_of(splits[0], (NF, NDIR, NLAT, NLON), ((0, 2), (2, 2), (3, 8)), -0.2, 0.2), 0.05, 1.0)
    group_speed = jnp.clip(jnp.exp(math.log(0.6) - 1.3862944 * jax.random.uniform(splits[1], (NF,), jnp.float32) ** steps_of(splits[1], (NF,), ((0, 2),), -0.2, 0.2)), 0.15, 0.6)
    sea_mask = place_ends((jax.random.randint(splits[2], (NLAT, NLON), 0, 4) < 3).astype(jnp.int32), jax.random.fold_in(splits[2], 1), 0, 1)
    wind_growth = jnp.clip(jnp.exp(math.log(2.0) - 2.3025851 * jax.random.uniform(splits[3], (NLAT, NLON), jnp.float32) ** steps_of(splits[3], (NLAT, NLON), ((0, 2), (1, 8)), -0.2, 0.2)), 0.2, 2.0)
    dissipation = jnp.clip(jnp.exp(math.log(1.0) - 2.3025851 * jax.random.uniform(splits[4], (NLAT, NLON), jnp.float32) ** steps_of(splits[4], (NLAT, NLON), ((0, 2), (1, 8)), -0.2, 0.2)), 0.1, 1.0)
    wind_profile = jnp.clip(jnp.exp(jax.random.uniform(splits[5], (NB,), jnp.float32, math.log(0.02), math.log(0.2))), 0.02, 0.2)
    nonlinear_coef = jnp.clip(jnp.exp(jax.random.uniform(splits[6], (NB,), jnp.float32, math.log(0.05), math.log(0.5))), 0.05, 0.5)
    momentum = noise(splits[7], (2, NB), 1.0, 6.0, jnp.float32)
    quadruplet = draw_quadruplet(jax.random.fold_in(splits[10], 71), 0)
    ocean_cell = draw_ocean_cell(jax.random.fold_in(splits[10], 71), 0)
    return {"spectrum": spectrum, "group_speed": group_speed, "sea_mask": sea_mask, "wind_growth": wind_growth, "dissipation": dissipation, "wind_profile": wind_profile, "nonlinear_coef": nonlinear_coef, "momentum": momentum, "quadruplet": quadruplet, "ocean_cell": ocean_cell}


time_step = 0.5


def propagate_all(spectrum, group_speed, sea_mask):
    ndirs = spectrum.shape[1]
    angles = 2.0 * jnp.pi * jnp.arange(ndirs).astype(jnp.float32) / ndirs
    speed_x = (group_speed[:, None] * jnp.cos(angles)[None, :])[:, :, None, None]
    speed_y = (group_speed[:, None] * jnp.sin(angles)[None, :])[:, :, None, None]
    west = jnp.roll(spectrum, 1, axis=3)
    east = jnp.roll(spectrum, -1, axis=3)
    padded = jnp.pad(spectrum, ((0, 0), (0, 0), (1, 1), (0, 0)))
    south = padded[:, :, :-2, :]
    north = padded[:, :, 2:, :]
    moved = (spectrum - jnp.maximum(speed_x, 0.0) * (spectrum - west) - jnp.minimum(speed_x, 0.0) * (east - spectrum)
             - jnp.maximum(speed_y, 0.0) * (spectrum - south) - jnp.minimum(speed_y, 0.0) * (north - spectrum))
    return moved * sea_mask.astype(jnp.float32)[None, None]


def reference(spectrum, group_speed, sea_mask, wind_growth, dissipation, wind_profile, nonlinear_coef, momentum, quadruplet, ocean_cell):
    highest = lax.Precision.HIGHEST
    moved = propagate_all(spectrum, group_speed, sea_mask)
    nbins = NF * NDIR
    flat_moved = moved.reshape(nbins, -1)
    weights = momentum * wind_profile[None, :]
    stress = jnp.dot(weights, flat_moved, precision=highest) * wind_growth.reshape(-1)[None, :]
    ocean_stress = jax.ops.segment_sum(stress.T, ocean_cell.reshape(-1), OCELLS)

    def one_row(packed):
        energy_row, wind_row, dissip_row, mask_row = packed
        flat_bins = energy_row.reshape(nbins, -1)
        third = flat_bins[quadruplet[0]]
        fourth = flat_bins[quadruplet[1]]
        transfer = nonlinear_coef[:, None] * (flat_bins * flat_bins * (third + fourth) - 2.0 * flat_bins * third * fourth)
        scattered = jnp.zeros_like(transfer).at[quadruplet[0]].add(transfer).at[quadruplet[1]].add(transfer)
        energy = jnp.mean(flat_bins, axis=0)
        tendency = (wind_row[None, :] * wind_profile[:, None] * flat_bins + scattered - 2.0 * transfer
                    - dissip_row[None, :] * energy[None, :] * flat_bins)
        result = mask_row[None, :] * (flat_bins + time_step * tendency)
        return result.reshape(energy_row.shape)

    by_rows = jnp.moveaxis(moved, 2, 0)
    updated = lax.map(one_row, (by_rows, wind_growth, dissipation, sea_mask.astype(jnp.float32)))
    spectrum_out = jnp.moveaxis(updated, 0, 2)
    return spectrum_out, ocean_stress
```

```python
import functools

import jax
import jax.numpy as jnp
import numpy as np
from jax import lax
from jax.experimental import pallas as pl
from jax.experimental.pallas import tpu as pltpu
from jax.sharding import PartitionSpec as P

time_step = 0.5
MESH = pl.DeviceIdType.MESH
VMEM = pltpu.VMEM


def spread(nf):
    order = list(range(4)) + list(range(nf - 4, nf)) + list(range(4, nf - 4))
    return {f: i for i, f in enumerate(order)}


def propagate_kernel(
    sizes, speed, spectrum, table, cols, mask, wind, cells,
    moved, energy, stress,
    x, pack_up, pack_down, got_up, got_down, edge_rows, lon_pack, got_left, got_right,
    part, parts,
    load_sem, lat_send, lat_recv, lon_send, lon_recv, freq_send, freq_recv, part_send, part_recv,
):
    n_lat, n_lon, n_freq, nf, nd, rows, nbins = sizes
    half = nd // 2
    pair = 2 * nd
    margin = 4 * nd
    band = nf * nd
    places = spread(nf)
    li, lo, fi = lax.axis_index("lat"), lax.axis_index("lon"), lax.axis_index("freq")
    load = pltpu.make_async_copy(spectrum, x, load_sem)
    load.start()

    east, west = lax.rem(lo + 1, n_lon), lax.rem(lo + n_lon - 1, n_lon)
    group = []
    for s in range(1, n_lat * n_freq):
        dl, df = divmod(s, n_freq)
        group.append(
            (dl, {"lat": lax.rem(li + dl, n_lat), "freq": lax.rem(fi + df, n_freq)})
        )
    barrier = pltpu.get_barrier_semaphore()
    for peer in [{"lon": east}, {"lon": west}] + [g for _, g in group]:
        pl.semaphore_signal(barrier, inc=1, device_id=peer, device_id_type=MESH)

    total_rows = pack_up.shape[0]
    pieces = ((0, 4 * half), (4 * half, 4 * half), (8 * half, total_rows - 8 * half))

    def lat_copy(k, up):
        at, size = pieces[k]
        src, dst = (pack_up, got_up) if up else (pack_down, got_down)
        i = k if up else 3 + k
        return pltpu.make_async_remote_copy(
            src.at[pl.ds(at, size)], dst.at[pl.ds(at, size)],
            lat_send.at[i], lat_recv.at[i],
            device_id={"lat": li + 1 if up else li - 1}, device_id_type=MESH,
        )

    def freq_copy(up):
        src = band if up else margin
        dst = 0 if up else margin + band
        return pltpu.make_async_remote_copy(
            moved.at[pl.ds(src, margin)], moved.at[pl.ds(dst, margin)],
            freq_send.at[int(up)], freq_recv.at[int(up)],
            device_id={"freq": fi + 1 if up else fi - 1}, device_id_type=MESH,
        )

    def lon_copy(to_east):
        return pltpu.make_async_remote_copy(
            lon_pack, got_left if to_east else got_right,
            lon_send.at[int(to_east)], lon_recv.at[int(to_east)],
            device_id={"lon": east if to_east else west}, device_id_type=MESH,
        )

    def part_copy(s):
        return pltpu.make_async_remote_copy(
            part, parts.at[s], part_send.at[s], part_recv.at[s],
            device_id=group[s][1], device_id_type=MESH,
        )

    up_ok, down_ok = li < n_lat - 1, li > 0
    pack_up[pl.ds(total_rows - 8, 8), :] = jnp.zeros((8, 128), jnp.float32)
    pack_down[pl.ds(total_rows - 8, 8), :] = jnp.zeros((8, 128), jnp.float32)
    load.wait()
    for f in range(nf):
        at = half * places[f]
        pack_up[pl.ds(at, half), :] = x[pl.ds(nd * f * rows + rows - 1, half, stride=rows), :]
        pack_down[pl.ds(at, half), :] = x[pl.ds((nd * f + half) * rows, half, stride=rows), :]
    pl.semaphore_wait(barrier, 2 + len(group))

    @pl.when(up_ok)
    def _():
        for k in range(3):
            lat_copy(k, True).start()

    @pl.when(down_ok)
    def _():
        for k in range(3):
            lat_copy(k, False).start()

    lane = lax.broadcasted_iota(jnp.int32, (pair, 128), 1)
    row = lax.broadcasted_iota(jnp.int32, (pair, 128), 0)
    row = jnp.where(row >= nd, row - nd, row)
    low = row < half
    cosine = table[pl.ds(0, pair), :]
    forward = cosine > 0.0
    rim = lane == jnp.where(forward, 0, 127)

    def shifted(e):
        return jnp.where(forward, pltpu.roll(e, 1, 1), pltpu.roll(e, 127, 1))

    def load_row(c, r):
        return x[pl.ds(pair * rows * c + r, pair, stride=rows), :]

    def pack_step(c, acc):
        for r in range(rows):
            z = jnp.where(rim, shifted(load_row(c, r)), 0.0)
            acc = acc + pltpu.roll(z, c * rows + r, 1)
        return acc

    lon_pack[...] = lax.fori_loop(0, nf // 2, pack_step, jnp.zeros((pair, 128), jnp.float32))
    lon_copy(True).start()
    lon_copy(False).start()

    @pl.when(jnp.logical_not(down_ok))
    def _():
        got_up[...] = jnp.zeros_like(got_up)

    @pl.when(jnp.logical_not(up_ok))
    def _():
        got_down[...] = jnp.zeros_like(got_down)

    @pl.when(fi == 0)
    def _():
        moved[pl.ds(0, margin), :] = jnp.zeros((margin, rows * 128), jnp.float32)

    @pl.when(fi == n_freq - 1)
    def _():
        moved[pl.ds(margin + band, margin), :] = jnp.zeros((margin, rows * 128), jnp.float32)

    def receive(k, freqs):
        @pl.when(down_ok)
        def _():
            lat_copy(k, True).wait_recv()

        @pl.when(up_ok)
        def _():
            lat_copy(k, False).wait_recv()

        for f in freqs:
            at = half * places[f]
            edge_rows[pl.ds(nd * f, half), :] = got_up[pl.ds(at, half), :]
            edge_rows[pl.ds(nd * f + half, half), :] = got_down[pl.ds(at, half), :]

    def chunk(c, sums):
        g = jnp.where(
            lax.broadcasted_iota(jnp.int32, (pair, 128), 0) < nd, speed[2 * c], speed[2 * c + 1]
        )
        ax = g * jnp.abs(table[pl.ds(0, pair), :])
        ay = g * jnp.abs(table[pl.ds(pair, pair), :])
        halo = jnp.where(forward, got_left[...], got_right[...])
        at = pl.multiple_of(pair * c, 8)
        outer = edge_rows[pl.ds(at, pair), :]
        here = pl.multiple_of(margin + pair * c, 8)
        w0 = cols[pl.ds(here, pair), 4:5]
        w1 = cols[pl.ds(here, pair), 5:6]
        e = [load_row(c, r) for r in range(rows)]
        out = []
        for r in range(rows):
            k = c * rows + r
            nx = jnp.where(rim, pltpu.roll(halo, 128 - k, 1), shifted(e[r]))
            below = e[r - 1] if r > 0 else outer
            above = e[r + 1] if r < rows - 1 else outer
            ny = jnp.where(low, below, above)
            m = (e[r] - ax * (e[r] - nx) - ay * (e[r] - ny)) * mask[r : r + 1, :].astype(jnp.float32)
            moved[pl.ds(here, pair), r * 128 : (r + 1) * 128] = m
            for i, v in enumerate((m, m * w0, m * w1)):
                s = sums[3 * r + i]
                for j in range(pair // 8):
                    s = s + v[8 * j : 8 * j + 8]
                out.append(s)
        return tuple(out)

    sums = tuple(jnp.zeros((8, 128), jnp.float32) for _ in range(3 * rows))
    lon_copy(True).wait_recv()
    lon_copy(False).wait_recv()
    receive(0, range(4))
    sums = lax.fori_loop(0, 2, chunk, sums)

    @pl.when(fi > 0)
    def _():
        freq_copy(False).start()

    receive(1, range(nf - 4, nf))
    sums = lax.fori_loop(nf // 2 - 2, nf // 2, chunk, sums)

    @pl.when(fi < n_freq - 1)
    def _():
        freq_copy(True).start()

    receive(2, range(4, nf - 4))
    sums = lax.fori_loop(2, nf // 2 - 2, chunk, sums)

    all_rows = n_lat * rows
    part[pl.ds(0, 8), :] = jnp.zeros((8, 128), jnp.float32)
    ids = (lo * 128 + lax.broadcasted_iota(jnp.int32, (all_rows, 128), 1)) * all_rows
    ids = ids + lax.broadcasted_iota(jnp.int32, (all_rows, 128), 0)
    totals = [jnp.zeros((all_rows, 128), jnp.float32) for _ in range(2)]
    for r in range(rows):
        part[r : r + 1, :] = jnp.sum(sums[3 * r], axis=0, keepdims=True)
        hit = cells[r : r + 1, :] == ids
        for i in range(2):
            tau = wind[r : r + 1, :] * jnp.sum(sums[3 * r + 1 + i], axis=0, keepdims=True)
            totals[i] = totals[i] + jnp.where(hit, tau, 0.0)
    for i in range(2):
        part[pl.ds(8 + i * all_rows, all_rows), :] = totals[i]
    for s in range(len(group)):
        part_copy(s).start()
    for s in range(len(group)):
        part_copy(s).wait()
    en = part[pl.ds(0, 8), :]
    st = part[pl.ds(8, 2 * all_rows), :]
    for s, (dl, _) in enumerate(group):
        if dl == 0:
            en = en + parts[s, pl.ds(0, 8), :]
        st = st + parts[s, pl.ds(8, 2 * all_rows), :]
    energy[...] = en / nbins
    stress[...] = pltpu.roll(st, lax.rem(128 - fi * (128 // n_freq), 128), 1)

    lon_copy(True).wait_send()
    lon_copy(False).wait_send()

    @pl.when(up_ok)
    def _():
        for k in range(3):
            lat_copy(k, True).wait_send()

    @pl.when(down_ok)
    def _():
        for k in range(3):
            lat_copy(k, False).wait_send()

    @pl.when(fi > 0)
    def _():
        freq_copy(False).wait_send()
        freq_copy(True).wait_recv()

    @pl.when(fi < n_freq - 1)
    def _():
        freq_copy(True).wait_send()
        freq_copy(False).wait_recv()


def split(v):
    high = v.astype(jnp.bfloat16)
    return high, (v - high.astype(jnp.float32)).astype(jnp.bfloat16)


def select_dot(pick, window):
    high, low = split(window)
    return jnp.dot(pick, high, preferred_element_type=jnp.float32) + jnp.dot(
        pick, low, preferred_element_type=jnp.float32
    )


def source_kernel(nf, nd, rows, moved, cols, lines, mask, wind, dissip, energy, out, trans):
    pair = 2 * nd
    chunks = nf // 2 + 4
    lane = lax.broadcasted_iota(jnp.int32, (pair, 3 * pair), 1)
    for c in range(1, chunks - 1):
        at = pair * c
        where = (lane + (at - pair)).astype(jnp.float32)
        picks = [
            jnp.where(cols[at : at + pair, i : i + 1] == where, 1.0, 0.0).astype(jnp.bfloat16)
            for i in range(2)
        ]
        both = select_dot(jnp.concatenate(picks, axis=0), moved[at - pair : at + 2 * pair, :])
        third, fourth = both[:pair], both[pair:]
        e = moved[at : at + pair, :]
        trans[at : at + pair, :] = cols[at : at + pair, 2:3] * (
            e * e * (third + fourth) - 2.0 * e * third * fourth
        )
    own = lax.broadcasted_iota(jnp.int32, (pair, 3 * pair), 0)
    for c in range(2, chunks - 2):
        at = pair * c
        window = trans[at - pair : at + 2 * pair, :]
        own_bin = (own + at).astype(jnp.float32)
        put = sum(
            jnp.where(lines[i : i + 1, at - pair : at + 2 * pair] == own_bin, 1.0, 0.0)
            for i in range(2)
        )
        back = select_dot(put.astype(jnp.bfloat16), window) - 2.0 * trans[at : at + pair, :]
        profile = cols[at : at + pair, 3:4]
        for r in range(rows):
            here = slice(r * 128, (r + 1) * 128)
            e = moved[at : at + pair, here]
            loss = dissip[r : r + 1, :] * energy[r : r + 1, :]
            tendency = wind[r : r + 1, :] * profile * e + back[:, here] - loss * e
            out[pl.ds(rows * (at - 2 * pair) + r, pair, stride=rows), :] = mask[
                r : r + 1, :
            ].astype(jnp.float32) * (e + time_step * tendency)


def local(
    axes,
    spectrum,
    group_speed,
    sea_mask,
    wind_growth,
    dissipation,
    wind_profile,
    nonlinear_coef,
    momentum,
    quadruplet,
    ocean_cell,
):
    n_lat, n_lon, n_freq = axes
    nf, nd, rows, width = spectrum.shape
    nbins = wind_profile.shape[0]
    band, margin, pair, half = nf * nd, 4 * nd, 2 * nd, nd // 2
    ext = band + 2 * margin
    all_rows = n_lat * rows
    f32 = jnp.float32
    angles = (np.float32(2.0 * np.pi) * np.arange(nd, dtype=np.float32) / np.float32(nd)).astype(
        np.float32
    )
    table = np.concatenate([np.tile(np.cos(angles), 2), np.tile(np.sin(angles), 2)])
    table = jnp.asarray(np.broadcast_to(table.astype(np.float32)[:, None], (2 * pair, width)))

    first = lax.axis_index("freq") * band
    lines = jnp.concatenate(
        [
            (quadruplet - (first - margin)).astype(f32),
            nonlinear_coef[None],
            wind_profile[None],
            momentum * wind_profile[None],
            jnp.zeros((2, nbins), f32),
        ]
    )
    lines = lax.dynamic_slice_in_dim(jnp.pad(lines, ((0, 0), (margin, margin))), first, ext, 1)
    cols = lines.T

    packed = -(-nf * half // 8) * 8
    peers = n_lat * n_freq - 1
    small = 8 + 2 * all_rows
    vmem = pl.BlockSpec(memory_space=VMEM)
    sizes = (n_lat, n_lon, n_freq, nf, nd, rows, nbins)
    dma = pltpu.SemaphoreType.DMA
    moved, energy, stress = pl.pallas_call(
        functools.partial(propagate_kernel, sizes),
        out_shape=(
            jax.ShapeDtypeStruct((ext, rows * width), f32),
            jax.ShapeDtypeStruct((8, width), f32),
            jax.ShapeDtypeStruct((2 * all_rows, width), f32),
        ),
        in_specs=[
            pl.BlockSpec(memory_space=pltpu.SMEM),
            pl.BlockSpec(memory_space=pl.ANY),
            vmem, vmem, vmem, vmem, vmem,
        ],
        out_specs=(vmem, vmem, vmem),
        scratch_shapes=[
            VMEM((band * rows, width), f32),
            VMEM((packed, width), f32),
            VMEM((packed, width), f32),
            VMEM((packed, width), f32),
            VMEM((packed, width), f32),
            VMEM((band, width), f32),
            VMEM((pair, width), f32),
            VMEM((pair, width), f32),
            VMEM((pair, width), f32),
            VMEM((small, width), f32),
            VMEM((peers, small, width), f32),
            dma, dma((6,)), dma((6,)), dma((2,)), dma((2,)), dma((2,)), dma((2,)),
            dma((peers,)), dma((peers,)),
        ],
        compiler_params=pltpu.CompilerParams(collective_id=0, has_side_effects=True),
    )(
        group_speed,
        spectrum.reshape(band * rows, width),
        table,
        cols,
        sea_mask,
        wind_growth,
        ocean_cell,
    )
    out = pl.pallas_call(
        functools.partial(source_kernel, nf, nd, rows),
        out_shape=jax.ShapeDtypeStruct((band * rows, width), f32),
        in_specs=[vmem] * 7,
        out_specs=vmem,
        scratch_shapes=[VMEM((ext, rows * width), f32)],
    )(moved, cols, lines, sea_mask, wind_growth, dissipation, energy)
    share = width // n_freq
    ocean = stress[:, :share].reshape(2, all_rows, share).transpose(2, 1, 0)
    return out.reshape(spectrum.shape), ocean.reshape(share * all_rows, 2)


def solution(mesh):
    axes = tuple(mesh.shape[a] for a in ("lat", "lon", "freq"))
    return jax.shard_map(
        functools.partial(local, axes),
        mesh=mesh,
        in_specs=(
            P("freq", None, "lat", "lon"),
            P("freq"),
            P("lat", "lon"),
            P("lat", "lon"),
            P("lat", "lon"),
            P(),
            P(),
            P(),
            P(),
            P("lat", "lon"),
        ),
        out_specs=(P("freq", None, "lat", "lon"), P(("lon", "freq"), None)),
        check_vma=False,
    )
```

```python
import functools

import jax
import jax.numpy as jnp
import numpy as np
from jax import lax
from jax.experimental import pallas as pl
from jax.experimental.pallas import tpu as pltpu
from jax.sharding import PartitionSpec as P

time_step = 0.5
MESH = pl.DeviceIdType.MESH
VMEM = pltpu.VMEM


def spread(nf):
    order = list(range(4)) + list(range(nf - 4, nf)) + list(range(4, nf - 4))
    return {f: i for i, f in enumerate(order)}


def propagate_kernel(
    sizes, speed, spectrum, waves, profile, coef, momentum, quad, mask, wind, dissip, cells,
    out, stress,
    x, moved, trans, result, table, cols, lines, pack_up, pack_down, got_up, got_down, edge_rows, lon_pack, got_left, got_right,
    part, parts,
    load_sem, store_sem, lat_send, lat_recv, lon_send, lon_recv, freq_send, freq_recv, part_send, part_recv,
):
    n_lat, n_lon, n_freq, nf, nd, rows, nbins = sizes
    half = nd // 2
    pair = 2 * nd
    margin = 4 * nd
    band = nf * nd
    places = spread(nf)
    li, lo, fi = lax.axis_index("lat"), lax.axis_index("lon"), lax.axis_index("freq")
    load = pltpu.make_async_copy(spectrum, x, load_sem)
    load.start()

    east, west = lax.rem(lo + 1, n_lon), lax.rem(lo + n_lon - 1, n_lon)
    group = []
    for s in range(1, n_lat * n_freq):
        dl, df = divmod(s, n_freq)
        group.append(
            (dl, {"lat": lax.rem(li + dl, n_lat), "freq": lax.rem(fi + df, n_freq)})
        )
    barrier = pltpu.get_barrier_semaphore()
    for peer in [{"lon": east}, {"lon": west}] + [g for _, g in group]:
        pl.semaphore_signal(barrier, inc=1, device_id=peer, device_id_type=MESH)

    total_rows = pack_up.shape[0]
    pieces = ((0, 4 * half), (4 * half, 4 * half), (8 * half, total_rows - 8 * half))

    def lat_copy(k, up):
        if isinstance(k, int):
            at, size = pieces[k]
        else:
            at, size = pl.multiple_of(k * (4 * half), 8), 4 * half
        src, dst = (pack_up, got_up) if up else (pack_down, got_down)
        i = k if up else 3 + k
        return pltpu.make_async_remote_copy(
            src.at[pl.ds(at, size)], dst.at[pl.ds(at, size)],
            lat_send.at[i], lat_recv.at[i],
            device_id={"lat": li + 1 if up else li - 1}, device_id_type=MESH,
        )

    def freq_copy(up):
        src = band if up else margin
        dst = 0 if up else margin + band
        return pltpu.make_async_remote_copy(
            moved.at[pl.ds(src, margin)], moved.at[pl.ds(dst, margin)],
            freq_send.at[int(up)], freq_recv.at[int(up)],
            device_id={"freq": fi + 1 if up else fi - 1}, device_id_type=MESH,
        )

    def lon_copy(to_east):
        return pltpu.make_async_remote_copy(
            lon_pack, got_left if to_east else got_right,
            lon_send.at[int(to_east)], lon_recv.at[int(to_east)],
            device_id={"lon": east if to_east else west}, device_id_type=MESH,
        )

    def part_copy(s):
        return pltpu.make_async_remote_copy(
            part, parts.at[s], part_send.at[s], part_recv.at[s],
            device_id=group[s][1], device_id_type=MESH,
        )

    up_ok, down_ok = li < n_lat - 1, li > 0
    near = lax.div(n_freq - fi, n_freq)
    order = (near, 1 - near, 2)

    span = lines.shape[1]
    lines[...] = jnp.zeros_like(lines)
    lines[0:2, 0:nbins] = (quad[...] - (fi * band - margin)).astype(jnp.float32)
    lines[2:3, 0:nbins] = coef[...].reshape(1, nbins)
    weight = profile[...].reshape(1, nbins)
    lines[3:4, 0:nbins] = weight
    lines[4:6, 0:nbins] = momentum[...] * weight
    lines[...] = pltpu.roll(lines[...], lax.rem(margin - fi * band + span, span), 1)
    for k in range(cols.shape[0] // 128):
        cols[pl.ds(128 * k, 128), :] = lines[:, 128 * k : 128 * k + 128].T
    turned = waves[...].T
    table[pl.ds(0, pair), :] = jnp.broadcast_to(turned[0:pair, 0:1], (pair, 128))
    table[pl.ds(pair, pair), :] = jnp.broadcast_to(turned[0:pair, 1:2], (pair, 128))

    pack_up[pl.ds(total_rows - 8, 8), :] = jnp.zeros((8, 128), jnp.float32)
    pack_down[pl.ds(total_rows - 8, 8), :] = jnp.zeros((8, 128), jnp.float32)
    load.wait()
    for f in range(nf):
        at = half * places[f]
        pack_up[pl.ds(at, half), :] = x[pl.ds(nd * f * rows + rows - 1, half, stride=rows), :]
        pack_down[pl.ds(at, half), :] = x[pl.ds((nd * f + half) * rows, half, stride=rows), :]

    lane = lax.broadcasted_iota(jnp.int32, (pair, 128), 1)
    row = lax.broadcasted_iota(jnp.int32, (pair, 128), 0)
    row = jnp.where(row >= nd, row - nd, row)
    low = row < half
    forward = table[pl.ds(0, pair), :] > 0.0
    rim = lane == jnp.where(forward, 0, 127)

    def shifted(e):
        return jnp.where(forward, pltpu.roll(e, 1, 1), pltpu.roll(e, 127, 1))

    def load_row(c, r):
        return x[pl.ds(pair * rows * c + r, pair, stride=rows), :]

    def pack_step(c, acc):
        for r in range(rows):
            z = jnp.where(rim, shifted(load_row(c, r)), 0.0)
            acc = acc + pltpu.roll(z, c * rows + r, 1)
        return acc

    lon_pack[...] = lax.fori_loop(0, nf // 2, pack_step, jnp.zeros((pair, 128), jnp.float32))
    pl.semaphore_wait(barrier, 2 + len(group))

    @pl.when(up_ok)
    def _():
        for k in order:
            lat_copy(k, True).start()

    @pl.when(down_ok)
    def _():
        for k in order:
            lat_copy(k, False).start()

    lon_copy(True).start()
    lon_copy(False).start()

    @pl.when(jnp.logical_not(down_ok))
    def _():
        got_up[...] = jnp.zeros_like(got_up)

    @pl.when(jnp.logical_not(up_ok))
    def _():
        got_down[...] = jnp.zeros_like(got_down)

    @pl.when(fi == 0)
    def _():
        moved[pl.ds(0, margin), :] = jnp.zeros((margin, rows * 128), jnp.float32)

    @pl.when(fi == n_freq - 1)
    def _():
        moved[pl.ds(margin + band, margin), :] = jnp.zeros((margin, rows * 128), jnp.float32)

    def receive(k, first, count):
        @pl.when(down_ok)
        def _():
            lat_copy(k, True).wait_recv()

        @pl.when(up_ok)
        def _():
            lat_copy(k, False).wait_recv()

        base = pieces[2][0] if isinstance(k, int) else pl.multiple_of(k * (4 * half), 8)
        for j in range(count):
            f, at = first + j, base + half * j
            edge_rows[pl.ds(nd * f, half), :] = got_up[pl.ds(at, half), :]
            edge_rows[pl.ds(nd * f + half, half), :] = got_down[pl.ds(at, half), :]

    def chunk(c, sums):
        g = jnp.where(
            lax.broadcasted_iota(jnp.int32, (pair, 128), 0) < nd, speed[2 * c], speed[2 * c + 1]
        )
        ax = g * jnp.abs(table[pl.ds(0, pair), :])
        ay = g * jnp.abs(table[pl.ds(pair, pair), :])
        halo = jnp.where(forward, got_left[...], got_right[...])
        at = pl.multiple_of(pair * c, 8)
        outer = edge_rows[pl.ds(at, pair), :]
        here = pl.multiple_of(margin + pair * c, 8)
        w0 = cols[pl.ds(here, pair), 4:5]
        w1 = cols[pl.ds(here, pair), 5:6]
        e = [load_row(c, r) for r in range(rows)]
        out = []
        for r in range(rows):
            k = c * rows + r
            nx = jnp.where(rim, pltpu.roll(halo, 128 - k, 1), shifted(e[r]))
            below = e[r - 1] if r > 0 else outer
            above = e[r + 1] if r < rows - 1 else outer
            ny = jnp.where(low, below, above)
            m = (e[r] - ax * (e[r] - nx) - ay * (e[r] - ny)) * mask[r : r + 1, :].astype(jnp.float32)
            moved[pl.ds(here, pair), r * 128 : (r + 1) * 128] = m
            for i, v in enumerate((m, m * w0, m * w1)):
                s = sums[3 * r + i]
                for j in range(pair // 8):
                    s = s + v[8 * j : 8 * j + 8]
                out.append(s)
        return tuple(out)

    sums = tuple(jnp.zeros((8, 128), jnp.float32) for _ in range(3 * rows))
    lon_copy(True).wait_recv()
    lon_copy(False).wait_recv()
    for k in (near, 1 - near):
        receive(k, k * (nf - 4), 4)
        sums = lax.fori_loop(k * (nf // 2 - 2), k * (nf // 2 - 2) + 2, chunk, sums)

        @pl.when(jnp.logical_and(k == 0, fi > 0))
        def _():
            freq_copy(False).start()

        @pl.when(jnp.logical_and(k == 1, fi < n_freq - 1))
        def _():
            freq_copy(True).start()

    receive(2, 4, nf - 8)
    sums = lax.fori_loop(2, nf // 2 - 2, chunk, sums)

    all_rows = n_lat * rows
    part[pl.ds(0, 8), :] = jnp.zeros((8, 128), jnp.float32)
    ids = (lo * 128 + lax.broadcasted_iota(jnp.int32, (all_rows, 128), 1)) * all_rows
    ids = ids + lax.broadcasted_iota(jnp.int32, (all_rows, 128), 0)
    totals = [jnp.zeros((all_rows, 128), jnp.float32) for _ in range(2)]
    for r in range(rows):
        part[r : r + 1, :] = jnp.sum(sums[3 * r], axis=0, keepdims=True)
        hit = cells[r : r + 1, :] == ids
        for i in range(2):
            tau = wind[r : r + 1, :] * jnp.sum(sums[3 * r + 1 + i], axis=0, keepdims=True)
            totals[i] = totals[i] + jnp.where(hit, tau, 0.0)
    for i in range(2):
        part[pl.ds(8 + i * all_rows, all_rows), :] = totals[i]
    for s in range(len(group)):
        part_copy(s).start()

    chunks = nf // 2 + 4
    is_low, is_high = fi == 0, fi == n_freq - 1
    t_from = jnp.where(is_low, 1, 3)
    t_to = jnp.where(is_high, chunks - 1, chunks - 3)
    o_from = jnp.where(is_low, 2, 4)
    o_to = jnp.where(is_high, chunks - 2, chunks - 4)
    lane3 = lax.broadcasted_iota(jnp.int32, (pair, 3 * pair), 1)
    row3 = lax.broadcasted_iota(jnp.int32, (pair, 3 * pair), 0)

    def interact(c, carry):
        at = pl.multiple_of(pair * c, 8)
        prior = pl.multiple_of(pair * c - pair, 8)
        where = (lane3 + prior).astype(jnp.float32)
        picks = [
            jnp.where(cols[pl.ds(at, pair), i : i + 1] == where, 1.0, 0.0).astype(jnp.bfloat16)
            for i in range(2)
        ]
        both = select_dot(jnp.concatenate(picks, axis=0), moved[pl.ds(prior, 3 * pair), :])
        third, fourth = both[:pair], both[pair:]
        e = moved[pl.ds(at, pair), :]
        trans[pl.ds(at, pair), :] = cols[pl.ds(at, pair), 2:3] * (
            e * e * (third + fourth) - 2.0 * e * third * fourth
        )
        return carry

    def store_copy(c):
        here = pl.ds(pl.multiple_of(rows * pair * (c - 2), 8), rows * pair)
        return pltpu.make_async_copy(result.at[here], out.at[here], store_sem.at[c - 2])

    def finish(c, carry):
        at = pl.multiple_of(pair * c, 8)
        prior = pl.multiple_of(pair * c - pair, 8)
        own_bin = (row3 + at).astype(jnp.float32)
        line = pltpu.roll(lines[...], span - prior, 1)
        put = jnp.where(line[0:1, : 3 * pair] == own_bin, 1.0, 0.0) + jnp.where(
            line[1:2, : 3 * pair] == own_bin, 1.0, 0.0
        )
        back = select_dot(put.astype(jnp.bfloat16), trans[pl.ds(prior, 3 * pair), :])
        back = back - 2.0 * trans[pl.ds(at, pair), :]
        shape = cols[pl.ds(at, pair), 3:4]
        for r in range(rows):
            here = slice(r * 128, (r + 1) * 128)
            e = moved[pl.ds(at, pair), here]
            loss = dissip[r : r + 1, :] * total_energy[r : r + 1, :]
            tendency = wind[r : r + 1, :] * shape * e + back[:, here] - loss * e
            result[pl.ds(rows * pair * (c - 2) + r, pair, stride=rows), :] = mask[
                r : r + 1, :
            ].astype(jnp.float32) * (e + time_step * tendency)
        store_copy(c).start()
        return carry

    lax.fori_loop(t_from, t_to, interact, 0)
    for s in range(len(group)):
        part_copy(s).wait()
    en = part[pl.ds(0, 8), :]
    st = part[pl.ds(8, 2 * all_rows), :]
    for s, (dl, _) in enumerate(group):
        if dl == 0:
            en = en + parts[s, pl.ds(0, 8), :]
        st = st + parts[s, pl.ds(8, 2 * all_rows), :]
    total_energy = en / nbins
    share = (128 // n_freq) * all_rows
    cell = lax.broadcasted_iota(jnp.int32, (128, share), 1)
    first_cell = (lax.broadcasted_iota(jnp.int32, (128, share), 0) - fi * (128 // n_freq)) * all_rows
    inside = jnp.logical_and(cell >= first_cell, cell < first_cell + all_rows)
    wide = jnp.dot(
        st, jnp.where(inside, 1.0, 0.0),
        precision=lax.Precision.HIGHEST, preferred_element_type=jnp.float32,
    )
    place = lax.broadcasted_iota(jnp.int32, (all_rows, share), 1) & (all_rows - 1)
    own_row = place == lax.broadcasted_iota(jnp.int32, (all_rows, share), 0)
    for i in range(2):
        picked = jnp.where(own_row, wide[i * all_rows : (i + 1) * all_rows], 0.0)
        stress[i : i + 1, :] = jnp.sum(picked, axis=0, keepdims=True)
    lax.fori_loop(o_from, o_to, finish, 0)

    @pl.when(fi > 0)
    def _():
        freq_copy(True).wait_recv()

    @pl.when(fi < n_freq - 1)
    def _():
        freq_copy(False).wait_recv()

    lax.fori_loop(1, t_from, interact, 0)
    lax.fori_loop(t_to, chunks - 1, interact, 0)
    lax.fori_loop(2, o_from, finish, 0)
    lax.fori_loop(o_to, chunks - 2, finish, 0)

    lon_copy(True).wait_send()
    lon_copy(False).wait_send()

    @pl.when(up_ok)
    def _():
        for k in range(3):
            lat_copy(k, True).wait_send()

    @pl.when(down_ok)
    def _():
        for k in range(3):
            lat_copy(k, False).wait_send()

    @pl.when(fi > 0)
    def _():
        freq_copy(False).wait_send()

    @pl.when(fi < n_freq - 1)
    def _():
        freq_copy(True).wait_send()

    for c in range(2, chunks - 2):
        store_copy(c).wait()


def split(v):
    high = v.astype(jnp.bfloat16)
    return high, (v - high.astype(jnp.float32)).astype(jnp.bfloat16)


def select_dot(pick, window):
    high, low = split(window)
    return jnp.dot(pick, high, preferred_element_type=jnp.float32) + jnp.dot(
        pick, low, preferred_element_type=jnp.float32
    )


def local(
    axes,
    spectrum,
    group_speed,
    sea_mask,
    wind_growth,
    dissipation,
    wind_profile,
    nonlinear_coef,
    momentum,
    quadruplet,
    ocean_cell,
):
    n_lat, n_lon, n_freq = axes
    nf, nd, rows, width = spectrum.shape
    nbins = wind_profile.shape[0]
    band, margin, pair, half = nf * nd, 4 * nd, 2 * nd, nd // 2
    ext = band + 2 * margin
    all_rows = n_lat * rows
    f32 = jnp.float32
    angles = (np.float32(2.0 * np.pi) * np.arange(nd, dtype=np.float32) / np.float32(nd)).astype(
        np.float32
    )
    waves = np.zeros((8, 128), np.float32)
    waves[0, :pair], waves[1, :pair] = np.tile(np.cos(angles), 2), np.tile(np.sin(angles), 2)

    packed = -(-nf * half // 8) * 8
    peers = n_lat * n_freq - 1
    small = 8 + 2 * all_rows
    share = (width // n_freq) * all_rows
    span = -(-(nbins + margin) // 128) * 128
    vmem = pl.BlockSpec(memory_space=VMEM)
    sizes = (n_lat, n_lon, n_freq, nf, nd, rows, nbins)
    dma = pltpu.SemaphoreType.DMA
    out, ocean = pl.pallas_call(
        functools.partial(propagate_kernel, sizes),
        out_shape=(
            jax.ShapeDtypeStruct((band * rows, width), f32),
            jax.ShapeDtypeStruct((2, share), f32),
        ),
        in_specs=[
            pl.BlockSpec(memory_space=pltpu.SMEM),
            pl.BlockSpec(memory_space=pl.ANY),
        ]
        + [vmem] * 9,
        out_specs=(pl.BlockSpec(memory_space=pl.ANY), vmem),
        scratch_shapes=[
            VMEM((band * rows, width), f32),
            VMEM((ext, rows * width), f32),
            VMEM((ext, rows * width), f32),
            VMEM((band * rows, width), f32),
            VMEM((2 * pair, width), f32),
            VMEM((-(-ext // 128) * 128, 8), f32),
            VMEM((8, span), f32),
            VMEM((packed, width), f32),
            VMEM((packed, width), f32),
            VMEM((packed, width), f32),
            VMEM((packed, width), f32),
            VMEM((band, width), f32),
            VMEM((pair, width), f32),
            VMEM((pair, width), f32),
            VMEM((pair, width), f32),
            VMEM((small, width), f32),
            VMEM((peers, small, width), f32),
            dma, dma((nf // 2,)),
            dma((6,)), dma((6,)), dma((2,)), dma((2,)), dma((2,)), dma((2,)),
            dma((peers,)), dma((peers,)),
        ],
        compiler_params=pltpu.CompilerParams(
            collective_id=0, has_side_effects=True, vmem_limit_bytes=24 << 20
        ),
    )(
        group_speed,
        spectrum.reshape(band * rows, width),
        jnp.asarray(waves),
        wind_profile,
        nonlinear_coef,
        momentum,
        quadruplet,
        sea_mask,
        wind_growth,
        dissipation,
        ocean_cell,
    )
    return out.reshape(spectrum.shape), ocean.T


def solution(mesh):
    axes = tuple(mesh.shape[a] for a in ("lat", "lon", "freq"))
    return jax.shard_map(
        functools.partial(local, axes),
        mesh=mesh,
        in_specs=(
            P("freq", None, "lat", "lon"),
            P("freq"),
            P("lat", "lon"),
            P("lat", "lon"),
            P("lat", "lon"),
            P(),
            P(),
            P(),
            P(),
            P("lat", "lon"),
        ),
        out_specs=(P("freq", None, "lat", "lon"), P(("lon", "freq"), None)),
        check_vma=False,
    )
```

```python
import functools

import jax
import jax.numpy as jnp
import numpy as np
from jax import lax
from jax.experimental import pallas as pl
from jax.experimental.pallas import tpu as pltpu
from jax.sharding import PartitionSpec as P

time_step = 0.5
MESH = pl.DeviceIdType.MESH
VMEM = pltpu.VMEM


def spread(nf):
    order = list(range(4)) + list(range(nf - 4, nf)) + list(range(4, nf - 4))
    return {f: i for i, f in enumerate(order)}


def propagate_kernel(
    sizes, spectrum, *refs
):
    sources, refs = refs[:10], refs[10:]
    out, stress, *refs = refs
    inputs, refs = refs[:10], refs[10:]
    speed, waves, profile, coef, momentum, quad, mask, wind, dissip, cells = inputs
    (
        x, moved, trans, result, table, rates, cols, lines, pack_up, pack_down, got_up, got_down,
        edge_rows, lon_pack, got_left, got_right, part, parts,
        load_sem, store_sem, small_sem, lat_send, lat_recv, lon_send, lon_recv, freq_send, freq_recv,
        part_send, part_recv,
    ) = refs
    n_lat, n_lon, n_freq, nf, nd, rows, nbins = sizes
    half = nd // 2
    pair = 2 * nd
    margin = 4 * nd
    band = nf * nd
    places = spread(nf)
    li, lo, fi = lax.axis_index("lat"), lax.axis_index("lon"), lax.axis_index("freq")
    load = pltpu.make_async_copy(spectrum, x, load_sem)
    load.start()
    small = [
        pltpu.make_async_copy(a, b, small_sem.at[i])
        for i, (a, b) in enumerate(zip(sources, inputs))
    ]
    for copy in small:
        copy.start()

    east, west = lax.rem(lo + 1, n_lon), lax.rem(lo + n_lon - 1, n_lon)
    group = []
    for s in range(1, n_lat * n_freq):
        dl, df = divmod(s, n_freq)
        group.append(
            (dl, {"lat": lax.rem(li + dl, n_lat), "freq": lax.rem(fi + df, n_freq)})
        )
    barrier = pltpu.get_barrier_semaphore()
    for peer in [{"lon": east}, {"lon": west}] + [g for _, g in group]:
        pl.semaphore_signal(barrier, inc=1, device_id=peer, device_id_type=MESH)

    total_rows = pack_up.shape[0]
    pieces = ((0, 4 * half), (4 * half, 4 * half), (8 * half, total_rows - 8 * half))

    def lat_copy(k, up):
        if isinstance(k, int):
            at, size = pieces[k]
        else:
            at, size = pl.multiple_of(k * (4 * half), 8), 4 * half
        src, dst = (pack_up, got_up) if up else (pack_down, got_down)
        i = k if up else 3 + k
        return pltpu.make_async_remote_copy(
            src.at[pl.ds(at, size)], dst.at[pl.ds(at, size)],
            lat_send.at[i], lat_recv.at[i],
            device_id={"lat": li + 1 if up else li - 1}, device_id_type=MESH,
        )

    def freq_copy(up):
        src = band if up else margin
        dst = 0 if up else margin + band
        return pltpu.make_async_remote_copy(
            moved.at[pl.ds(src, margin)], moved.at[pl.ds(dst, margin)],
            freq_send.at[int(up)], freq_recv.at[int(up)],
            device_id={"freq": fi + 1 if up else fi - 1}, device_id_type=MESH,
        )

    def lon_copy(to_east):
        return pltpu.make_async_remote_copy(
            lon_pack, got_left if to_east else got_right,
            lon_send.at[int(to_east)], lon_recv.at[int(to_east)],
            device_id={"lon": east if to_east else west}, device_id_type=MESH,
        )

    def part_copy(s):
        return pltpu.make_async_remote_copy(
            part, parts.at[s], part_send.at[s], part_recv.at[s],
            device_id=group[s][1], device_id_type=MESH,
        )

    up_ok, down_ok = li < n_lat - 1, li > 0
    near = lax.div(n_freq - fi, n_freq)
    order = (near, 1 - near, 2)

    for copy in small:
        copy.wait()
    span = lines.shape[1]
    rates[...] = jnp.zeros_like(rates)
    rates[0:1, 0:nf] = speed[...].reshape(1, nf)
    lines[...] = jnp.zeros_like(lines)
    lines[0:2, 0:nbins] = (quad[...] - (fi * band - margin)).astype(jnp.float32)
    lines[2:3, 0:nbins] = coef[...].reshape(1, nbins)
    weight = profile[...].reshape(1, nbins)
    lines[3:4, 0:nbins] = weight
    lines[4:6, 0:nbins] = momentum[...] * weight
    lines[...] = pltpu.roll(lines[...], lax.rem(margin - fi * band + span, span), 1)
    for k in range(cols.shape[0] // 128):
        cols[pl.ds(128 * k, 128), :] = lines[:, 128 * k : 128 * k + 128].T
    turned = waves[...].T
    table[pl.ds(0, pair), :] = jnp.broadcast_to(turned[0:pair, 0:1], (pair, 128))
    table[pl.ds(pair, pair), :] = jnp.broadcast_to(turned[0:pair, 1:2], (pair, 128))

    pack_up[pl.ds(total_rows - 8, 8), :] = jnp.zeros((8, 128), jnp.float32)
    pack_down[pl.ds(total_rows - 8, 8), :] = jnp.zeros((8, 128), jnp.float32)
    load.wait()
    for f in range(nf):
        at = half * places[f]
        pack_up[pl.ds(at, half), :] = x[pl.ds(nd * f * rows + rows - 1, half, stride=rows), :]
        pack_down[pl.ds(at, half), :] = x[pl.ds((nd * f + half) * rows, half, stride=rows), :]

    lane = lax.broadcasted_iota(jnp.int32, (pair, 128), 1)
    row = lax.broadcasted_iota(jnp.int32, (pair, 128), 0)
    row = jnp.where(row >= nd, row - nd, row)
    low = row < half
    forward = table[pl.ds(0, pair), :] > 0.0
    rim = lane == jnp.where(forward, 0, 127)

    def shifted(e):
        return jnp.where(forward, pltpu.roll(e, 1, 1), pltpu.roll(e, 127, 1))

    def load_row(c, r):
        return x[pl.ds(pair * rows * c + r, pair, stride=rows), :]

    def pack_step(c, acc):
        for r in range(rows):
            z = jnp.where(rim, shifted(load_row(c, r)), 0.0)
            acc = acc + pltpu.roll(z, c * rows + r, 1)
        return acc

    lon_pack[...] = lax.fori_loop(0, nf // 2, pack_step, jnp.zeros((pair, 128), jnp.float32))
    pl.semaphore_wait(barrier, 2 + len(group))

    @pl.when(up_ok)
    def _():
        for k in order:
            lat_copy(k, True).start()

    @pl.when(down_ok)
    def _():
        for k in order:
            lat_copy(k, False).start()

    lon_copy(True).start()
    lon_copy(False).start()

    @pl.when(jnp.logical_not(down_ok))
    def _():
        got_up[...] = jnp.zeros_like(got_up)

    @pl.when(jnp.logical_not(up_ok))
    def _():
        got_down[...] = jnp.zeros_like(got_down)

    @pl.when(fi == 0)
    def _():
        moved[pl.ds(0, margin), :] = jnp.zeros((margin, rows * 128), jnp.float32)

    @pl.when(fi == n_freq - 1)
    def _():
        moved[pl.ds(margin + band, margin), :] = jnp.zeros((margin, rows * 128), jnp.float32)

    def receive(k, first, count):
        @pl.when(down_ok)
        def _():
            lat_copy(k, True).wait_recv()

        @pl.when(up_ok)
        def _():
            lat_copy(k, False).wait_recv()

        base = pieces[2][0] if isinstance(k, int) else pl.multiple_of(k * (4 * half), 8)
        for j in range(count):
            f, at = first + j, base + half * j
            edge_rows[pl.ds(nd * f, half), :] = got_up[pl.ds(at, half), :]
            edge_rows[pl.ds(nd * f + half, half), :] = got_down[pl.ds(at, half), :]

    def chunk(c, sums):
        rate = pltpu.roll(rates[...], 128 - 2 * c, 1)
        g = jnp.where(
            lax.broadcasted_iota(jnp.int32, (pair, 128), 0) < nd,
            jnp.broadcast_to(rate[0:1, 0:1], (pair, 128)),
            jnp.broadcast_to(rate[0:1, 1:2], (pair, 128)),
        )
        ax = g * jnp.abs(table[pl.ds(0, pair), :])
        ay = g * jnp.abs(table[pl.ds(pair, pair), :])
        halo = jnp.where(forward, got_left[...], got_right[...])
        at = pl.multiple_of(pair * c, 8)
        outer = edge_rows[pl.ds(at, pair), :]
        here = pl.multiple_of(margin + pair * c, 8)
        w0 = cols[pl.ds(here, pair), 4:5]
        w1 = cols[pl.ds(here, pair), 5:6]
        e = [load_row(c, r) for r in range(rows)]
        out = []
        for r in range(rows):
            k = c * rows + r
            nx = jnp.where(rim, pltpu.roll(halo, 128 - k, 1), shifted(e[r]))
            below = e[r - 1] if r > 0 else outer
            above = e[r + 1] if r < rows - 1 else outer
            ny = jnp.where(low, below, above)
            m = (e[r] - ax * (e[r] - nx) - ay * (e[r] - ny)) * mask[r : r + 1, :].astype(jnp.float32)
            moved[pl.ds(here, pair), r * 128 : (r + 1) * 128] = m
            for i, v in enumerate((m, m * w0, m * w1)):
                s = sums[3 * r + i]
                for j in range(pair // 8):
                    s = s + v[8 * j : 8 * j + 8]
                out.append(s)
        return tuple(out)

    sums = tuple(jnp.zeros((8, 128), jnp.float32) for _ in range(3 * rows))
    lon_copy(True).wait_recv()
    lon_copy(False).wait_recv()
    for k in (near, 1 - near):
        receive(k, k * (nf - 4), 4)
        sums = lax.fori_loop(k * (nf // 2 - 2), k * (nf // 2 - 2) + 2, chunk, sums)

        @pl.when(jnp.logical_and(k == 0, fi > 0))
        def _():
            freq_copy(False).start()

        @pl.when(jnp.logical_and(k == 1, fi < n_freq - 1))
        def _():
            freq_copy(True).start()

    receive(2, 4, nf - 8)
    sums = lax.fori_loop(2, nf // 2 - 2, chunk, sums)

    all_rows = n_lat * rows
    part[pl.ds(0, 8), :] = jnp.zeros((8, 128), jnp.float32)
    ids = (lo * 128 + lax.broadcasted_iota(jnp.int32, (all_rows, 128), 1)) * all_rows
    ids = ids + lax.broadcasted_iota(jnp.int32, (all_rows, 128), 0)
    totals = [jnp.zeros((all_rows, 128), jnp.float32) for _ in range(2)]
    for r in range(rows):
        part[r : r + 1, :] = jnp.sum(sums[3 * r], axis=0, keepdims=True)
        hit = cells[r : r + 1, :] == ids
        for i in range(2):
            tau = wind[r : r + 1, :] * jnp.sum(sums[3 * r + 1 + i], axis=0, keepdims=True)
            totals[i] = totals[i] + jnp.where(hit, tau, 0.0)
    for i in range(2):
        part[pl.ds(8 + i * all_rows, all_rows), :] = totals[i]
    for s in range(len(group)):
        part_copy(s).start()

    chunks = nf // 2 + 4
    is_low, is_high = fi == 0, fi == n_freq - 1
    t_from = jnp.where(is_low, 1, 3)
    t_to = jnp.where(is_high, chunks - 1, chunks - 3)
    o_from = jnp.where(is_low, 2, 4)
    o_to = jnp.where(is_high, chunks - 2, chunks - 4)
    lane3 = lax.broadcasted_iota(jnp.int32, (pair, 3 * pair), 1)
    row3 = lax.broadcasted_iota(jnp.int32, (pair, 3 * pair), 0)

    def interact(c, carry):
        at = pl.multiple_of(pair * c, 8)
        prior = pl.multiple_of(pair * c - pair, 8)
        where = (lane3 + prior).astype(jnp.float32)
        picks = [
            jnp.where(cols[pl.ds(at, pair), i : i + 1] == where, 1.0, 0.0).astype(jnp.bfloat16)
            for i in range(2)
        ]
        both = select_dot(jnp.concatenate(picks, axis=0), moved[pl.ds(prior, 3 * pair), :])
        third, fourth = both[:pair], both[pair:]
        e = moved[pl.ds(at, pair), :]
        trans[pl.ds(at, pair), :] = cols[pl.ds(at, pair), 2:3] * (
            e * e * (third + fourth) - 2.0 * e * third * fourth
        )
        return carry

    def store_copy(c):
        here = pl.ds(pl.multiple_of(rows * pair * (c - 2), 8), rows * pair)
        return pltpu.make_async_copy(result.at[here], out.at[here], store_sem.at[c - 2])

    def finish(c, carry):
        at = pl.multiple_of(pair * c, 8)
        prior = pl.multiple_of(pair * c - pair, 8)
        own_bin = (row3 + at).astype(jnp.float32)
        line = pltpu.roll(lines[...], span - prior, 1)
        put = jnp.where(line[0:1, : 3 * pair] == own_bin, 1.0, 0.0) + jnp.where(
            line[1:2, : 3 * pair] == own_bin, 1.0, 0.0
        )
        back = select_dot(put.astype(jnp.bfloat16), trans[pl.ds(prior, 3 * pair), :])
        back = back - 2.0 * trans[pl.ds(at, pair), :]
        shape = cols[pl.ds(at, pair), 3:4]
        for r in range(rows):
            here = slice(r * 128, (r + 1) * 128)
            e = moved[pl.ds(at, pair), here]
            loss = dissip[r : r + 1, :] * total_energy[r : r + 1, :]
            tendency = wind[r : r + 1, :] * shape * e + back[:, here] - loss * e
            result[pl.ds(rows * pair * (c - 2) + r, pair, stride=rows), :] = mask[
                r : r + 1, :
            ].astype(jnp.float32) * (e + time_step * tendency)
        store_copy(c).start()
        return carry

    lax.fori_loop(t_from, t_to, interact, 0)
    for s in range(len(group)):
        part_copy(s).wait()
    en = part[pl.ds(0, 8), :]
    st = part[pl.ds(8, 2 * all_rows), :]
    for s, (dl, _) in enumerate(group):
        if dl == 0:
            en = en + parts[s, pl.ds(0, 8), :]
        st = st + parts[s, pl.ds(8, 2 * all_rows), :]
    total_energy = en / nbins
    share = (128 // n_freq) * all_rows
    cell = lax.broadcasted_iota(jnp.int32, (128, share), 1)
    first_cell = (lax.broadcasted_iota(jnp.int32, (128, share), 0) - fi * (128 // n_freq)) * all_rows
    inside = jnp.logical_and(cell >= first_cell, cell < first_cell + all_rows)
    wide = jnp.dot(
        st, jnp.where(inside, 1.0, 0.0),
        precision=lax.Precision.HIGHEST, preferred_element_type=jnp.float32,
    )
    place = lax.broadcasted_iota(jnp.int32, (all_rows, share), 1) & (all_rows - 1)
    own_row = place == lax.broadcasted_iota(jnp.int32, (all_rows, share), 0)
    for i in range(2):
        picked = jnp.where(own_row, wide[i * all_rows : (i + 1) * all_rows], 0.0)
        stress[i : i + 1, :] = jnp.sum(picked, axis=0, keepdims=True)
    lax.fori_loop(o_from, o_to, finish, 0)

    @pl.when(fi > 0)
    def _():
        freq_copy(True).wait_recv()

    @pl.when(fi < n_freq - 1)
    def _():
        freq_copy(False).wait_recv()

    lax.fori_loop(1, t_from, interact, 0)
    lax.fori_loop(t_to, chunks - 1, interact, 0)
    lax.fori_loop(2, o_from, finish, 0)
    lax.fori_loop(o_to, chunks - 2, finish, 0)

    lon_copy(True).wait_send()
    lon_copy(False).wait_send()

    @pl.when(up_ok)
    def _():
        for k in range(3):
            lat_copy(k, True).wait_send()

    @pl.when(down_ok)
    def _():
        for k in range(3):
            lat_copy(k, False).wait_send()

    @pl.when(fi > 0)
    def _():
        freq_copy(False).wait_send()

    @pl.when(fi < n_freq - 1)
    def _():
        freq_copy(True).wait_send()

    for c in range(2, chunks - 2):
        store_copy(c).wait()


def split(v):
    high = v.astype(jnp.bfloat16)
    return high, (v - high.astype(jnp.float32)).astype(jnp.bfloat16)


def select_dot(pick, window):
    high, low = split(window)
    return jnp.dot(pick, high, preferred_element_type=jnp.float32) + jnp.dot(
        pick, low, preferred_element_type=jnp.float32
    )


def local(
    axes,
    spectrum,
    group_speed,
    sea_mask,
    wind_growth,
    dissipation,
    wind_profile,
    nonlinear_coef,
    momentum,
    quadruplet,
    ocean_cell,
):
    n_lat, n_lon, n_freq = axes
    nf, nd, rows, width = spectrum.shape
    nbins = wind_profile.shape[0]
    band, margin, pair, half = nf * nd, 4 * nd, 2 * nd, nd // 2
    ext = band + 2 * margin
    all_rows = n_lat * rows
    f32 = jnp.float32
    angles = (np.float32(2.0 * np.pi) * np.arange(nd, dtype=np.float32) / np.float32(nd)).astype(
        np.float32
    )
    waves = np.zeros((8, 128), np.float32)
    waves[0, :pair], waves[1, :pair] = np.tile(np.cos(angles), 2), np.tile(np.sin(angles), 2)

    packed = -(-nf * half // 8) * 8
    peers = n_lat * n_freq - 1
    small = 8 + 2 * all_rows
    share = (width // n_freq) * all_rows
    span = -(-(nbins + margin) // 128) * 128
    vmem = pl.BlockSpec(memory_space=VMEM)
    sizes = (n_lat, n_lon, n_freq, nf, nd, rows, nbins)
    dma = pltpu.SemaphoreType.DMA
    smalls = (
        group_speed,
        jnp.asarray(waves),
        wind_profile,
        nonlinear_coef,
        momentum,
        quadruplet,
        sea_mask,
        wind_growth,
        dissipation,
        ocean_cell,
    )
    out, ocean = pl.pallas_call(
        functools.partial(propagate_kernel, sizes),
        out_shape=(
            jax.ShapeDtypeStruct((band * rows, width), f32),
            jax.ShapeDtypeStruct((2, share), f32),
        ),
        in_specs=[pl.BlockSpec(memory_space=pltpu.HBM)] * 11,
        out_specs=(pl.BlockSpec(memory_space=pltpu.HBM), vmem),
        scratch_shapes=[VMEM(a.shape, a.dtype) for a in smalls]
        + [
            VMEM((band * rows, width), f32),
            VMEM((ext, rows * width), f32),
            VMEM((ext, rows * width), f32),
            VMEM((band * rows, width), f32),
            VMEM((2 * pair, width), f32),
            VMEM((8, width), f32),
            VMEM((-(-ext // 128) * 128, 8), f32),
            VMEM((8, span), f32),
            VMEM((packed, width), f32),
            VMEM((packed, width), f32),
            VMEM((packed, width), f32),
            VMEM((packed, width), f32),
            VMEM((band, width), f32),
            VMEM((pair, width), f32),
            VMEM((pair, width), f32),
            VMEM((pair, width), f32),
            VMEM((small, width), f32),
            VMEM((peers, small, width), f32),
            dma, dma((nf // 2,)), dma((len(smalls),)),
            dma((6,)), dma((6,)), dma((2,)), dma((2,)), dma((2,)), dma((2,)),
            dma((peers,)), dma((peers,)),
        ],
        compiler_params=pltpu.CompilerParams(
            collective_id=0, has_side_effects=True
        ),
    )(spectrum.reshape(band * rows, width), *smalls)
    return out.reshape(spectrum.shape), ocean.T


def solution(mesh):
    axes = tuple(mesh.shape[a] for a in ("lat", "lon", "freq"))
    return jax.shard_map(
        functools.partial(local, axes),
        mesh=mesh,
        in_specs=(
            P("freq", None, "lat", "lon"),
            P("freq"),
            P("lat", "lon"),
            P("lat", "lon"),
            P("lat", "lon"),
            P(),
            P(),
            P(),
            P(),
            P("lat", "lon"),
        ),
        out_specs=(P("freq", None, "lat", "lon"), P(("lon", "freq"), None)),
        check_vma=False,
    )
```

```python
import functools

import jax
import jax.numpy as jnp
import numpy as np
from jax import lax
from jax.experimental import pallas as pl
from jax.experimental.pallas import tpu as pltpu
from jax.sharding import PartitionSpec as P

time_step = 0.5
MESH = pl.DeviceIdType.MESH
VMEM = pltpu.VMEM


def spread(nf):
    order = list(range(4)) + list(range(nf - 4, nf)) + list(range(4, nf - 4))
    return {f: i for i, f in enumerate(order)}


def propagate_kernel(
    sizes, spectrum, *refs
):
    sources, refs = refs[:10], refs[10:]
    result, stress, *refs = refs
    inputs, refs = refs[:10], refs[10:]
    speed, waves, profile, coef, momentum, quad, mask, wind, dissip, cells = inputs
    (
        x, moved, trans, table, rates, cols, lines, pack_up, pack_down, got_up, got_down,
        edge_rows, lon_pack, got_left, got_right, part, parts,
        load_sem, small_sem, lat_send, lat_recv, lon_send, lon_recv, freq_send, freq_recv,
        part_send, part_recv,
    ) = refs
    n_lat, n_lon, n_freq, nf, nd, rows, nbins = sizes
    half = nd // 2
    pair = 2 * nd
    margin = 4 * nd
    band = nf * nd
    places = spread(nf)
    li, lo, fi = lax.axis_index("lat"), lax.axis_index("lon"), lax.axis_index("freq")
    load = pltpu.make_async_copy(spectrum, x, load_sem)
    load.start()
    small = [
        pltpu.make_async_copy(a, b, small_sem.at[i])
        for i, (a, b) in enumerate(zip(sources, inputs))
    ]
    for copy in small:
        copy.start()

    east, west = lax.rem(lo + 1, n_lon), lax.rem(lo + n_lon - 1, n_lon)
    group = []
    for s in range(1, n_lat * n_freq):
        dl, df = divmod(s, n_freq)
        group.append(
            (dl, {"lat": lax.rem(li + dl, n_lat), "freq": lax.rem(fi + df, n_freq)})
        )
    barrier = pltpu.get_barrier_semaphore()
    for peer in [{"lon": east}, {"lon": west}] + [g for _, g in group]:
        pl.semaphore_signal(barrier, inc=1, device_id=peer, device_id_type=MESH)

    total_rows = pack_up.shape[0]
    pieces = ((0, 4 * half), (4 * half, 4 * half), (8 * half, total_rows - 8 * half))

    def lat_copy(k, up):
        if isinstance(k, int):
            at, size = pieces[k]
        else:
            at, size = pl.multiple_of(k * (4 * half), 8), 4 * half
        src, dst = (pack_up, got_up) if up else (pack_down, got_down)
        i = k if up else 3 + k
        return pltpu.make_async_remote_copy(
            src.at[pl.ds(at, size)], dst.at[pl.ds(at, size)],
            lat_send.at[i], lat_recv.at[i],
            device_id={"lat": li + 1 if up else li - 1}, device_id_type=MESH,
        )

    def freq_copy(up):
        src = band if up else margin
        dst = 0 if up else margin + band
        return pltpu.make_async_remote_copy(
            moved.at[pl.ds(src, margin)], moved.at[pl.ds(dst, margin)],
            freq_send.at[int(up)], freq_recv.at[int(up)],
            device_id={"freq": fi + 1 if up else fi - 1}, device_id_type=MESH,
        )

    def lon_copy(to_east):
        return pltpu.make_async_remote_copy(
            lon_pack, got_left if to_east else got_right,
            lon_send.at[int(to_east)], lon_recv.at[int(to_east)],
            device_id={"lon": east if to_east else west}, device_id_type=MESH,
        )

    def part_copy(s):
        return pltpu.make_async_remote_copy(
            part, parts.at[s], part_send.at[s], part_recv.at[s],
            device_id=group[s][1], device_id_type=MESH,
        )

    up_ok, down_ok = li < n_lat - 1, li > 0
    near = lax.div(n_freq - fi, n_freq)
    order = (near, 1 - near, 2)

    for copy in small:
        copy.wait()
    span = lines.shape[1]
    rates[...] = jnp.zeros_like(rates)
    rates[0:1, 0:nf] = speed[...].reshape(1, nf)
    lines[...] = jnp.zeros_like(lines)
    lines[0:2, 0:nbins] = (quad[...] - (fi * band - margin)).astype(jnp.float32)
    lines[2:3, 0:nbins] = coef[...].reshape(1, nbins)
    weight = profile[...].reshape(1, nbins)
    lines[3:4, 0:nbins] = weight
    lines[4:6, 0:nbins] = momentum[...] * weight
    lines[...] = pltpu.roll(lines[...], lax.rem(margin - fi * band + span, span), 1)
    for k in range(cols.shape[0] // 128):
        cols[pl.ds(128 * k, 128), :] = lines[:, 128 * k : 128 * k + 128].T
    turned = waves[...].T
    table[pl.ds(0, pair), :] = jnp.broadcast_to(turned[0:pair, 0:1], (pair, 128))
    table[pl.ds(pair, pair), :] = jnp.broadcast_to(turned[0:pair, 1:2], (pair, 128))

    pack_up[pl.ds(total_rows - 8, 8), :] = jnp.zeros((8, 128), jnp.float32)
    pack_down[pl.ds(total_rows - 8, 8), :] = jnp.zeros((8, 128), jnp.float32)
    load.wait()
    for f in range(nf):
        at = half * places[f]
        pack_up[pl.ds(at, half), :] = x[pl.ds(nd * f * rows + rows - 1, half, stride=rows), :]
        pack_down[pl.ds(at, half), :] = x[pl.ds((nd * f + half) * rows, half, stride=rows), :]

    lane = lax.broadcasted_iota(jnp.int32, (pair, 128), 1)
    row = lax.broadcasted_iota(jnp.int32, (pair, 128), 0)
    row = jnp.where(row >= nd, row - nd, row)
    low = row < half
    forward = table[pl.ds(0, pair), :] > 0.0
    rim = lane == jnp.where(forward, 0, 127)
    sent = lane == jnp.where(forward, 127, 0)

    def shifted(e):
        return jnp.where(forward, pltpu.roll(e, 1, 1), pltpu.roll(e, 127, 1))

    def load_row(c, r):
        return x[pl.ds(pair * rows * c + r, pair, stride=rows), :]

    def pack_step(c, acc):
        for r in range(rows):
            z = jnp.where(sent, load_row(c, r), 0.0)
            acc = acc + pltpu.roll(z, c * rows + r, 1)
        return acc

    lon_pack[...] = lax.fori_loop(0, nf // 2, pack_step, jnp.zeros((pair, 128), jnp.float32))
    pl.semaphore_wait(barrier, 2 + len(group))

    @pl.when(up_ok)
    def _():
        for k in order:
            lat_copy(k, True).start()

    @pl.when(down_ok)
    def _():
        for k in order:
            lat_copy(k, False).start()

    lon_copy(True).start()
    lon_copy(False).start()

    @pl.when(jnp.logical_not(down_ok))
    def _():
        got_up[...] = jnp.zeros_like(got_up)

    @pl.when(jnp.logical_not(up_ok))
    def _():
        got_down[...] = jnp.zeros_like(got_down)

    @pl.when(fi == 0)
    def _():
        moved[pl.ds(0, margin), :] = jnp.zeros((margin, rows * 128), jnp.float32)

    @pl.when(fi == n_freq - 1)
    def _():
        moved[pl.ds(margin + band, margin), :] = jnp.zeros((margin, rows * 128), jnp.float32)

    def receive(k, first, count):
        @pl.when(down_ok)
        def _():
            lat_copy(k, True).wait_recv()

        @pl.when(up_ok)
        def _():
            lat_copy(k, False).wait_recv()

        base = pieces[2][0] if isinstance(k, int) else pl.multiple_of(k * (4 * half), 8)
        for j in range(count):
            f, at = first + j, base + half * j
            edge_rows[pl.ds(nd * f, half), :] = got_up[pl.ds(at, half), :]
            edge_rows[pl.ds(nd * f + half, half), :] = got_down[pl.ds(at, half), :]

    def chunk(c, sums):
        rate = pltpu.roll(rates[...], 128 - 2 * c, 1)
        g = jnp.where(
            lax.broadcasted_iota(jnp.int32, (pair, 128), 0) < nd,
            jnp.broadcast_to(rate[0:1, 0:1], (pair, 128)),
            jnp.broadcast_to(rate[0:1, 1:2], (pair, 128)),
        )
        ax = g * jnp.abs(table[pl.ds(0, pair), :])
        ay = g * jnp.abs(table[pl.ds(pair, pair), :])
        halo = got_left[...]
        at = pl.multiple_of(pair * c, 8)
        outer = edge_rows[pl.ds(at, pair), :]
        here = pl.multiple_of(margin + pair * c, 8)
        w0 = cols[pl.ds(here, pair), 4:5]
        w1 = cols[pl.ds(here, pair), 5:6]
        e = [load_row(c, r) for r in range(rows)]
        out = []
        for r in range(rows):
            k = c * rows + r
            nx = jnp.where(rim, pltpu.roll(halo, 128 - k, 1), shifted(e[r]))
            below = e[r - 1] if r > 0 else outer
            above = e[r + 1] if r < rows - 1 else outer
            ny = jnp.where(low, below, above)
            m = (e[r] - ax * (e[r] - nx) - ay * (e[r] - ny)) * mask[r : r + 1, :].astype(jnp.float32)
            moved[pl.ds(here, pair), r * 128 : (r + 1) * 128] = m
            for i, v in enumerate((m, m * w0, m * w1)):
                s = sums[3 * r + i]
                for j in range(pair // 8):
                    s = s + v[8 * j : 8 * j + 8]
                out.append(s)
        return tuple(out)

    sums = tuple(jnp.zeros((8, 128), jnp.float32) for _ in range(3 * rows))
    lon_copy(True).wait_recv()
    lon_copy(False).wait_recv()
    got_left[...] = jnp.where(
        forward, pltpu.roll(got_left[...], 1, 1), pltpu.roll(got_right[...], 127, 1)
    )
    for k in (near, 1 - near):
        receive(k, k * (nf - 4), 4)
        sums = lax.fori_loop(k * (nf // 2 - 2), k * (nf // 2 - 2) + 2, chunk, sums)

        @pl.when(jnp.logical_and(k == 0, fi > 0))
        def _():
            freq_copy(False).start()

        @pl.when(jnp.logical_and(k == 1, fi < n_freq - 1))
        def _():
            freq_copy(True).start()

    receive(2, 4, nf - 8)
    sums = lax.fori_loop(2, nf // 2 - 2, chunk, sums)

    all_rows = n_lat * rows
    part[pl.ds(0, 8), :] = jnp.zeros((8, 128), jnp.float32)
    ids = (lo * 128 + lax.broadcasted_iota(jnp.int32, (all_rows, 128), 1)) * all_rows
    ids = ids + lax.broadcasted_iota(jnp.int32, (all_rows, 128), 0)
    totals = [jnp.zeros((all_rows, 128), jnp.float32) for _ in range(2)]
    for r in range(rows):
        part[r : r + 1, :] = jnp.sum(sums[3 * r], axis=0, keepdims=True)
        hit = cells[r : r + 1, :] == ids
        for i in range(2):
            tau = wind[r : r + 1, :] * jnp.sum(sums[3 * r + 1 + i], axis=0, keepdims=True)
            totals[i] = totals[i] + jnp.where(hit, tau, 0.0)
    for i in range(2):
        part[pl.ds(8 + i * all_rows, all_rows), :] = totals[i]
    for s in range(len(group)):
        part_copy(s).start()

    chunks = nf // 2 + 4
    is_low, is_high = fi == 0, fi == n_freq - 1
    t_from = jnp.where(is_low, 1, 3)
    t_to = jnp.where(is_high, chunks - 1, chunks - 3)
    o_from = jnp.where(is_low, 2, 4)
    o_to = jnp.where(is_high, chunks - 2, chunks - 4)
    lane3 = lax.broadcasted_iota(jnp.int32, (pair, 3 * pair), 1)
    row3 = lax.broadcasted_iota(jnp.int32, (pair, 3 * pair), 0)

    def interact(c, carry):
        at = pl.multiple_of(pair * c, 8)
        prior = pl.multiple_of(pair * c - pair, 8)
        where = (lane3 + prior).astype(jnp.float32)
        picks = [
            jnp.where(cols[pl.ds(at, pair), i : i + 1] == where, 1.0, 0.0).astype(jnp.bfloat16)
            for i in range(2)
        ]
        both = select_dot(jnp.concatenate(picks, axis=0), moved[pl.ds(prior, 3 * pair), :])
        third, fourth = both[:pair], both[pair:]
        e = moved[pl.ds(at, pair), :]
        trans[pl.ds(at, pair), :] = cols[pl.ds(at, pair), 2:3] * (
            e * e * (third + fourth) - 2.0 * e * third * fourth
        )
        return carry

    def finish(c, carry):
        at = pl.multiple_of(pair * c, 8)
        prior = pl.multiple_of(pair * c - pair, 8)
        own_bin = (row3 + at).astype(jnp.float32)
        line = pltpu.roll(lines[...], span - prior, 1)
        put = jnp.where(line[0:1, : 3 * pair] == own_bin, 1.0, 0.0) + jnp.where(
            line[1:2, : 3 * pair] == own_bin, 1.0, 0.0
        )
        back = select_dot(put.astype(jnp.bfloat16), trans[pl.ds(prior, 3 * pair), :])
        back = back - 2.0 * trans[pl.ds(at, pair), :]
        shape = cols[pl.ds(at, pair), 3:4]
        for r in range(rows):
            here = slice(r * 128, (r + 1) * 128)
            e = moved[pl.ds(at, pair), here]
            loss = dissip[r : r + 1, :] * total_energy[r : r + 1, :]
            tendency = wind[r : r + 1, :] * shape * e + back[:, here] - loss * e
            result[pl.ds(rows * pair * (c - 2) + r, pair, stride=rows), :] = mask[
                r : r + 1, :
            ].astype(jnp.float32) * (e + time_step * tendency)
        return carry

    lax.fori_loop(t_from, t_to, interact, 0)
    for s in range(len(group)):
        part_copy(s).wait()
    en = part[pl.ds(0, 8), :]
    st = part[pl.ds(8, 2 * all_rows), :]
    for s, (dl, _) in enumerate(group):
        if dl == 0:
            en = en + parts[s, pl.ds(0, 8), :]
        st = st + parts[s, pl.ds(8, 2 * all_rows), :]
    total_energy = en / nbins
    share = (128 // n_freq) * all_rows
    cell = lax.broadcasted_iota(jnp.int32, (128, share), 1)
    first_cell = (lax.broadcasted_iota(jnp.int32, (128, share), 0) - fi * (128 // n_freq)) * all_rows
    inside = jnp.logical_and(cell >= first_cell, cell < first_cell + all_rows)
    wide = jnp.dot(
        st, jnp.where(inside, 1.0, 0.0),
        precision=lax.Precision.HIGHEST, preferred_element_type=jnp.float32,
    )
    place = lax.broadcasted_iota(jnp.int32, (all_rows, share), 1) & (all_rows - 1)
    own_row = place == lax.broadcasted_iota(jnp.int32, (all_rows, share), 0)
    for i in range(2):
        picked = jnp.where(own_row, wide[i * all_rows : (i + 1) * all_rows], 0.0)
        stress[i : i + 1, :] = jnp.sum(picked, axis=0, keepdims=True)
    lax.fori_loop(o_from, o_to, finish, 0)

    @pl.when(fi > 0)
    def _():
        freq_copy(True).wait_recv()

    @pl.when(fi < n_freq - 1)
    def _():
        freq_copy(False).wait_recv()

    lax.fori_loop(1, t_from, interact, 0)
    lax.fori_loop(t_to, chunks - 1, interact, 0)
    lax.fori_loop(2, o_from, finish, 0)
    lax.fori_loop(o_to, chunks - 2, finish, 0)

    lon_copy(True).wait_send()
    lon_copy(False).wait_send()

    @pl.when(up_ok)
    def _():
        for k in range(3):
            lat_copy(k, True).wait_send()

    @pl.when(down_ok)
    def _():
        for k in range(3):
            lat_copy(k, False).wait_send()

    @pl.when(fi > 0)
    def _():
        freq_copy(False).wait_send()

    @pl.when(fi < n_freq - 1)
    def _():
        freq_copy(True).wait_send()

def split(v):
    high = v.astype(jnp.bfloat16)
    return high, (v - high.astype(jnp.float32)).astype(jnp.bfloat16)


def select_dot(pick, window):
    high, low = split(window)
    return jnp.dot(pick, high, preferred_element_type=jnp.float32) + jnp.dot(
        pick, low, preferred_element_type=jnp.float32
    )


def local(
    axes,
    spectrum,
    group_speed,
    sea_mask,
    wind_growth,
    dissipation,
    wind_profile,
    nonlinear_coef,
    momentum,
    quadruplet,
    ocean_cell,
):
    n_lat, n_lon, n_freq = axes
    nf, nd, rows, width = spectrum.shape
    nbins = wind_profile.shape[0]
    band, margin, pair, half = nf * nd, 4 * nd, 2 * nd, nd // 2
    ext = band + 2 * margin
    all_rows = n_lat * rows
    f32 = jnp.float32
    angles = (np.float32(2.0 * np.pi) * np.arange(nd, dtype=np.float32) / np.float32(nd)).astype(
        np.float32
    )
    waves = np.zeros((8, 128), np.float32)
    waves[0, :pair], waves[1, :pair] = np.tile(np.cos(angles), 2), np.tile(np.sin(angles), 2)

    packed = -(-nf * half // 8) * 8
    peers = n_lat * n_freq - 1
    small = 8 + 2 * all_rows
    share = (width // n_freq) * all_rows
    span = -(-(nbins + margin) // 128) * 128
    vmem = pl.BlockSpec(memory_space=VMEM)
    sizes = (n_lat, n_lon, n_freq, nf, nd, rows, nbins)
    dma = pltpu.SemaphoreType.DMA
    smalls = (
        group_speed,
        jnp.asarray(waves),
        wind_profile,
        nonlinear_coef,
        momentum,
        quadruplet,
        sea_mask,
        wind_growth,
        dissipation,
        ocean_cell,
    )
    out, ocean = pl.pallas_call(
        functools.partial(propagate_kernel, sizes),
        out_shape=(
            jax.ShapeDtypeStruct((band * rows, width), f32),
            jax.ShapeDtypeStruct((2, share), f32),
        ),
        in_specs=[pl.BlockSpec(memory_space=pltpu.HBM)] * 11,
        out_specs=(vmem, vmem),
        scratch_shapes=[VMEM(a.shape, a.dtype) for a in smalls]
        + [
            VMEM((band * rows, width), f32),
            VMEM((ext, rows * width), f32),
            VMEM((ext, rows * width), f32),
            VMEM((2 * pair, width), f32),
            VMEM((8, width), f32),
            VMEM((-(-ext // 128) * 128, 8), f32),
            VMEM((8, span), f32),
            VMEM((packed, width), f32),
            VMEM((packed, width), f32),
            VMEM((packed, width), f32),
            VMEM((packed, width), f32),
            VMEM((band, width), f32),
            VMEM((pair, width), f32),
            VMEM((pair, width), f32),
            VMEM((pair, width), f32),
            VMEM((small, width), f32),
            VMEM((peers, small, width), f32),
            dma, dma((len(smalls),)),
            dma((6,)), dma((6,)), dma((2,)), dma((2,)), dma((2,)), dma((2,)),
            dma((peers,)), dma((peers,)),
        ],
        compiler_params=pltpu.CompilerParams(
            collective_id=0, has_side_effects=True, vmem_limit_bytes=24 << 20
        ),
    )(
        *[
            pltpu.with_memory_space_constraint(a, pltpu.HBM)
            for a in (spectrum.reshape(band * rows, width), *smalls)
        ]
    )
    return out.reshape(spectrum.shape), ocean.T


def solution(mesh):
    axes = tuple(mesh.shape[a] for a in ("lat", "lon", "freq"))
    return jax.shard_map(
        functools.partial(local, axes),
        mesh=mesh,
        in_specs=(
            P("freq", None, "lat", "lon"),
            P("freq"),
            P("lat", "lon"),
            P("lat", "lon"),
            P("lat", "lon"),
            P(),
            P(),
            P(),
            P(),
            P("lat", "lon"),
        ),
        out_specs=(P("freq", None, "lat", "lon"), P(("lon", "freq"), None)),
        check_vma=False,
    )
```
